32 devices in a mesh: seq: 8 (over z, core), tp: 4 (over y, x).
Axes of the slice: x: 2, y: 2, z: 4, core: 2. Of those that a mesh axis runs over, the one named last changes fastest.
Arguments:
- hidden_in: bfloat16 [4096, 4608], P('seq'), may hold values from -6 to 6
- pre_gain: float32 [4608], replicated, may hold values from 0.5 to 1.5
- w_query: bfloat16 [4608, 4096], P(None, 'tp'), may hold values from -0.09375 to 0.09375
- key_cache: bfloat16 [8192, 2048], P('seq', 'tp'), may hold values from -12 to 12
- value_cache: bfloat16 [8192, 2048], P('seq', 'tp'), may hold values from -6 to 6
- w_out: bfloat16 [4096, 4608], P('tp'), may hold values from -0.75 to 0.75
- post_gain: float32 [4608], replicated, may hold values from 0.5 to 1.5
- starts: int32 [8], replicated, may hold values from 0 to 7680, as said below
- counts: int32 [8], replicated, may hold values from 512 to 1024, as said below
Outputs:
- layer_out: bfloat16 [4096, 4608], P(('seq', 'tp'))
The draws below stay inside these ranges and needn't reach their ends.
Inputs may be any that keep to these rules, and one draw needn't show every extreme that they name: The queries of shard s sit at positions starts[s] to starts[s] + 511, all inside the filled rows of shard s, that is from s * 1024 to s * 1024 + counts[s] - 1. `counts`: at least one shard is full.
All inputs are finite; a program needn't handle non-finite values.
Results may differ from the reference program's by a relative error of at most 0.012.
Values may be sent and summed in bfloat16 or wider, within the bound.
No kernel may reach another device: no remote copies, remote signals or barrier semaphores. Data moves between devices by JAX's collectives and lax.ppermute only.
A program may use at most 128 MiB of HBM per device.

```python
import jax
import jax.numpy as jnp
from jax import lax

D = 4608
H = 32
KVH = 16
HD = 128
WINDOW = 4096
CTX_DEV = 1024
Q_DEV = 512
HALO = 4
CONTEXT = 8192
TOKENS = 4096
N_SEQ = 8
N_TP = 4


def fill_table(key):
    count_key = jax.random.fold_in(key, 11)
    full_key = jax.random.fold_in(key, 12)
    offset_key = jax.random.fold_in(key, 13)
    shard_ids = jnp.arange(N_SEQ, dtype=jnp.int32)
    counts = jax.random.randint(count_key, (N_SEQ,), Q_DEV, CTX_DEV + 1, dtype=jnp.int32)
    full_shard = jax.random.randint(full_key, (), 0, N_SEQ, dtype=jnp.int32)
    counts = jnp.where(shard_ids == full_shard, jnp.int32(CTX_DEV), counts)
    offsets = jax.random.randint(offset_key, (N_SEQ,), 0, counts - Q_DEV + 1, dtype=jnp.int32)
    starts = shard_ids * CTX_DEV + offsets
    return (starts.astype(jnp.int32), counts.astype(jnp.int32))


def draw_starts(key, part):
    return fill_table(key)[0]


def draw_counts(key, part):
    return fill_table(key)[1]


def levels(rng, shape, shards, least, top_value):
    def one(axis_at, blocks):
        draws = jax.random.uniform(jax.random.fold_in(jax.random.fold_in(rng, 6), axis_at), (blocks,), jnp.float32, least / len(shards), top_value / len(shards))
        return jnp.repeat(jnp.exp(draws), shape[axis_at] // blocks).reshape((-1,) + (1,) * (len(shape) - axis_at - 1))

    level = one(*shards[0])
    for cut in shards[1:]:
        level = level * one(*cut)
    return level


def gaussian(key, shape, scale, reach, shards=(), kind=jnp.bfloat16):
    gain = levels(key, shape, shards, -0.22, 0.18) if shards else 1.0
    result = jax.random.normal(key, shape, jnp.float32) * scale * gain
    return jnp.minimum(jnp.maximum(result, -reach), reach).astype(kind)


def setup_inputs(seed: int = 0) -> dict:
    seeds = jax.random.split(jax.random.key(seed), 10)
    hidden_in = gaussian(seeds[0], (TOKENS, D), 1.0, 6.0, ((0, 8),))
    pre_gain = jnp.clip(1.0 + 0.1 * jax.random.normal(seeds[1], (D,), jnp.float32), 0.5, 1.5)
    w_query = gaussian(seeds[2], (D, H * HD), D ** -0.5, 0.09375, ((1, 4),))
    key_cache = gaussian(seeds[3], (CONTEXT, KVH * HD), 2.0, 12.0, ((0, 8), (1, 4)))
    value_cache = gaussian(seeds[4], (CONTEXT, KVH * HD), 1.0, 6.0, ((0, 8), (1, 4)))
    w_out = gaussian(seeds[5], (H * HD, D), (H * HD // 64) ** -0.5, 0.75, ((0, 4),))
    post_gain = jnp.clip(1.0 + 0.1 * jax.random.normal(seeds[6], (D,), jnp.float32), 0.5, 1.5)
    starts = draw_starts(jax.random.fold_in(seeds[9], 71), 0)
    counts = draw_counts(jax.random.fold_in(seeds[9], 71), 0)
    return dict(hidden_in=hidden_in, pre_gain=pre_gain, w_query=w_query, key_cache=key_cache, value_cache=value_cache, w_out=w_out, post_gain=post_gain, starts=starts, counts=counts)


def reference(hidden_in, pre_gain, w_query, key_cache, value_cache, w_out, post_gain, starts, counts):
    per_group = H // KVH
    key_span = (HALO + 1) * CTX_DEV
    inputs = hidden_in.astype(jnp.float32)
    normed = (inputs * lax.rsqrt(lax.optimization_barrier(jnp.mean(inputs * inputs, axis=-1, keepdims=True)) + 0.1) * pre_gain).astype(jnp.bfloat16)
    queries = (jnp.dot(normed, w_query, preferred_element_type=jnp.float32) * (D // H) ** (-0.5)).astype(jnp.bfloat16)
    padding = jnp.zeros((HALO * CTX_DEV, KVH * HD), jnp.bfloat16)
    keys_padded = jnp.concatenate([padding, key_cache], axis=0)
    values_padded = jnp.concatenate([padding, value_cache], axis=0)
    w_groups = w_out.astype(jnp.float32).reshape(N_TP, H * HD // N_TP, D)

    def one_shard(shard):
        shard = shard.astype(jnp.int32)
        query_block = lax.dynamic_slice_in_dim(queries, (shard * Q_DEV).astype(jnp.int32), Q_DEV, 0)
        key_block = lax.dynamic_slice_in_dim(keys_padded, (shard * CTX_DEV).astype(jnp.int32), key_span, 0)
        value_block = lax.dynamic_slice_in_dim(values_padded, (shard * CTX_DEV).astype(jnp.int32), key_span, 0)
        key_pos = (shard - HALO) * CTX_DEV + jnp.arange(key_span, dtype=jnp.int32)
        source = jnp.clip(key_pos // CTX_DEV, 0, N_SEQ - 1).astype(jnp.int32)
        filled = (key_pos >= 0) & (key_pos - source * CTX_DEV < counts[source])
        query_pos = starts[shard] + jnp.arange(Q_DEV, dtype=jnp.int32)
        allowed = filled[None, :] & (key_pos[None, :] <= query_pos[:, None]) & (key_pos[None, :] > query_pos[:, None] - WINDOW)
        query_f = lax.optimization_barrier(query_block).astype(jnp.float32).reshape(Q_DEV, KVH, per_group, HD)
        key_f = key_block.astype(jnp.float32).reshape(key_span, KVH, HD)
        value_f = value_block.astype(jnp.float32).reshape(key_span, KVH, HD)
        scores = jnp.einsum('qkgd,ckd->kgqc', query_f, key_f, precision=lax.Precision.HIGHEST)
        scores = 50.0 * jnp.tanh(scores / 50.0)
        weight = jnp.where(allowed[None, None], jnp.exp(scores), jnp.float32(0.0))
        denominator = lax.optimization_barrier(jnp.sum(weight, axis=-1))
        weight16 = lax.optimization_barrier(weight.astype(jnp.bfloat16)).astype(jnp.float32)
        context = jnp.einsum('kgqc,ckd->qkgd', weight16, value_f, precision=lax.Precision.HIGHEST)
        attended = (context / jnp.transpose(denominator, (2, 0, 1))[..., None]).reshape(Q_DEV, H * HD).astype(jnp.bfloat16)
        attended_f = lax.optimization_barrier(attended).astype(jnp.float32).reshape(Q_DEV, N_TP, H * HD // N_TP)
        partial_value = jnp.einsum('qtf,tfd->tqd', attended_f, w_groups, precision=lax.Precision.HIGHEST)
        partial_value = lax.optimization_barrier(partial_value.astype(jnp.bfloat16)).astype(jnp.float32)
        projected = lax.optimization_barrier(jnp.sum(partial_value, axis=0))
        residual = lax.dynamic_slice_in_dim(hidden_in, (shard * Q_DEV).astype(jnp.int32), Q_DEV, 0).astype(jnp.float32)
        mixed = residual + projected * lax.rsqrt(lax.optimization_barrier(jnp.mean(projected * projected, axis=-1, keepdims=True)) + 0.1) * post_gain
        return mixed.astype(jnp.bfloat16)
    layer_out = lax.map(one_shard, jnp.arange(N_SEQ, dtype=jnp.int32))
    return layer_out.reshape(N_SEQ * Q_DEV, D)
```

```python
import functools

import jax
import jax.numpy as jnp
from jax import lax
from jax.experimental import pallas as pl
from jax.experimental.pallas import tpu as pltpu
from jax.sharding import PartitionSpec as P

D = 4608
H = 32
HD = 128
WINDOW = 4096
HALO = 4
KEY_CHUNK = 1024
QUERY_TILE = 128
EXPONENT = 50.0 * 1.4426950408889634


def attend_kernel(
    kind, per_group, meta, q_ref, k_ref, v_ref, *refs
):
    if kind == "own":
        num_out, den_out, q_all, acc = refs
    elif kind == "mid":
        num_in, den_in, num_out, den_out, q_all, acc = refs
    else:
        num_in, den_in, out_ref, q_all, acc = refs
    group = pl.program_id(0)
    rows = q_ref.shape[0]
    first, last, query_at, filled = meta[0], meta[1], meta[2], meta[3]
    for g in range(per_group):
        q_all[g * rows : (g + 1) * rows, :] = q_ref[:, g * HD : (g + 1) * HD]
    acc[...] = jnp.zeros_like(acc)

    def chunk(c, carry):
        at = c * KEY_CHUNK
        keys = k_ref[pl.ds(at, KEY_CHUNK), :]
        values = v_ref[pl.ds(at, KEY_CHUNK), :]
        row = at + lax.broadcasted_iota(jnp.int32, (KEY_CHUNK, HD), 0)
        kept = (row < filled).astype(jnp.float32).astype(jnp.bfloat16)
        wide = jnp.concatenate([values * kept, kept], axis=1)
        tiles = per_group * rows // QUERY_TILE

        def scored(t):
            return lax.dot_general(
                q_all[t * QUERY_TILE : (t + 1) * QUERY_TILE, :],
                keys,
                (((1,), (1,)), ((), ())),
                preferred_element_type=jnp.float32,
            )

        coming = scored(0)
        for t in range(tiles):
            scores = coming
            if t + 1 < tiles:
                coming = scored(t + 1)
            span = slice(t * QUERY_TILE, (t + 1) * QUERY_TILE)
            weight = jnp.exp2(EXPONENT * jnp.tanh(scores * (1.0 / 50.0)))
            if kind != "mid":
                shape = (QUERY_TILE, KEY_CHUNK)
                query = lax.broadcasted_iota(jnp.int32, shape, 0)
                key = lax.broadcasted_iota(jnp.int32, shape, 1)
                gap = query_at + (t * QUERY_TILE) % rows - at
                ahead = key - query
                seen = ahead <= gap if kind == "own" else ahead > gap
                weight = jnp.where(seen, weight, 0.0)
            acc[span, :] += jnp.dot(
                weight.astype(jnp.bfloat16), wide, preferred_element_type=jnp.float32
            )
        return carry

    lax.fori_loop(first, last, chunk, 0)
    lane = lax.broadcasted_iota(jnp.int32, (rows, HD), 1)
    if kind == "own":
        den = jnp.where(group == 0, 0.0, den_out[...])
    elif kind == "mid":
        den = jnp.where(group == 0, den_in[...], den_out[...])
    for g in range(per_group):
        head = group * per_group + g
        span = slice(g * rows, (g + 1) * rows)
        cols = slice(g * HD, (g + 1) * HD)
        if kind == "own":
            num_out[:, cols] = acc[span, :HD]
            den = jnp.where(lane == head, acc[span, HD:], den)
        elif kind == "mid":
            num_out[:, cols] = num_in[:, cols] + acc[span, :HD]
            den = den + jnp.where(lane == head, acc[span, HD:], 0.0)
        else:
            before = jnp.sum(
                jnp.where(lane == head, den_in[...], 0.0), axis=1, keepdims=True
            )
            total = before + acc[span, HD:]
            out_ref[:, cols] = ((num_in[:, cols] + acc[span, :HD]) / total).astype(
                jnp.bfloat16
            )
    if kind != "last":
        den_out[...] = den


def attend(kind, meta, queries, keys, values, running):
    rows, width = queries.shape
    cache_rows = keys.shape[0]
    kv_local = keys.shape[1] // HD
    per_group = width // HD // kv_local
    wide = per_group * HD
    head_block = lambda n, w: pl.BlockSpec((n, w), lambda j, m: (0, j))
    den_block = pl.BlockSpec((rows, HD), lambda j, m: (0, 0))
    in_specs = [
        head_block(rows, wide),
        head_block(cache_rows, HD),
        head_block(cache_rows, HD),
    ]
    args = [queries, keys, values]
    aliases = {}
    if kind != "own":
        in_specs += [head_block(rows, wide), den_block]
        args += list(running)
    if kind == "last":
        out_shape = jax.ShapeDtypeStruct((rows, width), jnp.bfloat16)
        out_specs = head_block(rows, wide)
    else:
        out_shape = (
            jax.ShapeDtypeStruct((rows, width), jnp.float32),
            jax.ShapeDtypeStruct((rows, HD), jnp.float32),
        )
        out_specs = (head_block(rows, wide), den_block)
    if kind == "mid":
        aliases = {4: 0, 5: 1}
    return pl.pallas_call(
        functools.partial(attend_kernel, kind, per_group),
        out_shape=out_shape,
        grid_spec=pltpu.PrefetchScalarGridSpec(
            num_scalar_prefetch=1,
            grid=(kv_local,),
            in_specs=in_specs,
            out_specs=out_specs,
            scratch_shapes=[
                pltpu.VMEM((per_group * rows, HD), jnp.bfloat16),
                pltpu.VMEM((per_group * rows, 2 * HD), jnp.float32),
            ],
        ),
        input_output_aliases=aliases,
        compiler_params=pltpu.CompilerParams(
            dimension_semantics=("arbitrary",), vmem_limit_bytes=24 * 2**20
        ),
        cost_estimate=pl.CostEstimate(
            flops=4 * rows * cache_rows * width * 2,
            transcendentals=2 * rows * cache_rows * width // HD,
            bytes_accessed=8 * rows * width,
        ),
        name="attend_" + kind,
    )(meta, *args)


def passed_along(block, axis, distance):
    devices = range(lax.axis_size(axis))
    route = [(i - distance, i) for i in devices if i - distance in devices]
    return lax.ppermute(block, axis, route)


def picked(block, bits, bit, value):
    at = bits.index(bit)
    rows = block.shape[0]
    split = block.reshape(2**at, 2, rows // 2 ** (at + 1), block.shape[1])
    return lax.dynamic_index_in_dim(split, value, 1, keepdims=False).reshape(
        rows // 2, block.shape[1]
    )


def swapped(block, bit):
    count = lax.axis_size("tp")
    return lax.ppermute(block, "tp", [(i, i ^ (1 << bit)) for i in range(count)])


def scattered(attended, weights):
    count = lax.axis_size("tp")
    place = lax.axis_index("tp")
    high_first = list(range(count.bit_length() - 1))[::-1]
    orders = [high_first[::-1], high_first]
    left = [list(high_first) for _ in orders]
    state = [None] * len(orders)
    for step in range(len(high_first)):
        sent = []
        for n, order in enumerate(orders):
            bit = order[step]
            mine = (place >> bit) & 1
            if step == 0:
                away = jnp.dot(
                    picked(attended, left[n], bit, 1 - mine),
                    weights[n],
                    preferred_element_type=jnp.float32,
                )
            else:
                away = picked(state[n], left[n], bit, 1 - mine)
            sent.append(swapped(away.astype(jnp.bfloat16), bit))
        for n, order in enumerate(orders):
            bit = order[step]
            mine = (place >> bit) & 1
            if step == 0:
                kept = lax.optimization_barrier(
                    jnp.dot(
                        picked(attended, left[n], bit, mine),
                        weights[n],
                        preferred_element_type=jnp.float32,
                    )
                )
            else:
                kept = picked(state[n], left[n], bit, mine)
            state[n] = kept + sent[n].astype(jnp.float32)
            left[n].remove(bit)
    return state


def shards(hidden_in, pre_gain, w_query, key_cache, value_cache, w_out, post_gain, starts, counts):
    seq_count = lax.axis_size("seq")
    own_shard = lax.axis_index("seq")
    query_rows = hidden_in.shape[0]
    cache_rows = key_cache.shape[0]
    moved = [(key_cache, value_cache)]

    inputs = hidden_in.astype(jnp.float32)
    normed = (
        inputs * lax.rsqrt(jnp.mean(inputs * inputs, axis=-1, keepdims=True) + 0.1) * pre_gain
    ).astype(jnp.bfloat16)
    queries = (
        jnp.dot(normed, w_query, preferred_element_type=jnp.float32) * (D // H) ** (-0.5)
    ).astype(jnp.bfloat16)

    query_at = lax.dynamic_index_in_dim(starts, own_shard, 0, keepdims=False) - own_shard * cache_rows
    sources = own_shard - jnp.arange(HALO + 1, dtype=jnp.int32)
    filled = jnp.where(sources >= 0, counts[jnp.clip(sources, 0, seq_count - 1)], 0)
    places = jnp.arange(HALO + 1)
    first = jnp.where(places == HALO, (query_at + 1) // KEY_CHUNK, 0)
    reach = jnp.where(places == 0, query_at + query_rows, filled)
    last = (reach + KEY_CHUNK - 1) // KEY_CHUNK
    meta = jnp.stack([first, last, jnp.full_like(first, query_at), filled], axis=1).astype(jnp.int32)

    running = None
    done = []
    for distance in range(HALO + 1):
        kind = "own" if distance == 0 else "last" if distance == HALO else "mid"
        keys, values = moved[distance]
        if distance < HALO:
            if distance == 1:
                keys, _ = lax.optimization_barrier((keys, normed))
                values, _ = lax.optimization_barrier((values, queries))
            elif distance > 1:
                keys, _ = lax.optimization_barrier((keys, done[0 if distance == 2 else distance - 1]))
                values, _ = lax.optimization_barrier((values, done[distance - 1]))
            moved.append((passed_along(keys, "seq", 1), passed_along(values, "seq", 1)))
        running = attend(kind, meta[distance], queries, keys, values, running)
        done.append(running[1] if distance < HALO else None)
    attended = running

    block_rows = query_rows // lax.axis_size("tp")
    tp_place = lax.axis_index("tp")
    width = w_out.shape[1]
    half = width // 2
    projected = scattered(attended, [w_out[:, :half], w_out[:, half:]])
    residual = lax.dynamic_slice_in_dim(hidden_in, tp_place * block_rows, block_rows, 0).astype(jnp.float32)
    square = sum(jnp.sum(p * p, axis=-1, keepdims=True) for p in projected)
    scale = lax.rsqrt(square / width + 0.1)
    mixed = [
        residual[:, n * half : (n + 1) * half]
        + p * scale * post_gain[n * half : (n + 1) * half]
        for n, p in enumerate(projected)
    ]
    return jnp.concatenate(mixed, axis=1).astype(jnp.bfloat16)


def solution(mesh):
    return jax.shard_map(
        shards,
        mesh=mesh,
        in_specs=(
            P("seq", None),
            P(),
            P(None, "tp"),
            P("seq", "tp"),
            P("seq", "tp"),
            P("tp", None),
            P(),
            P(),
            P(),
        ),
        out_specs=P(("seq", "tp"), None),
        check_vma=False,
    )
```
